32 devices in a mesh: grp: 2 (over y), gx: 4 (over z), gy: 2 (over x), gz: 2 (over core).
Axes of the slice: x: 2, y: 2, z: 4, core: 2. Of those that a mesh axis runs over, the one named last changes fastest.
Arguments:
- alignment_token_ids: int32 [128, 128], P(('grp', 'gx'), ('gy', 'gz')), parts along dimension 0, may hold values from 0 to 22
- homolog_profile: bfloat16 [128, 128, 256], P(('grp', 'gx'), ('gy', 'gz')), parts along dimension 0, may hold values from -6 to 6
- alignment_mask: int32 [128, 128], P(('grp', 'gx'), ('gy', 'gz')), parts along dimension 0, may hold values 0 or 1
- pair_features: bfloat16 [256, 128, 128], P(('grp', 'gy', 'gz'), 'gx'), parts along dimension 0, may hold values from -4 to 6
- symbol_lookup_weights: bfloat16 [23, 256], replicated, may hold values from -6 to 6
- asking_weights: bfloat16 [256, 256], replicated, may hold values from -0.375 to 0.375
- lookup_weights: bfloat16 [256, 256], replicated, may hold values from -0.375 to 0.375
- content_weights: bfloat16 [256, 256], replicated, may hold values from -0.375 to 0.375
- sigmoid_switch_weights: bfloat16 [256, 256], replicated, may hold values from -0.375 to 0.375
- resulting_weights: bfloat16 [256, 256], replicated, may hold values from -0.75 to 0.75
- pair_bias_matrix: float32 [128, 8], replicated, may hold values from -0.9 to 48
- first_factor_weights: bfloat16 [256, 32], replicated, may hold values from -0.375 to 0.375
- second_factor_weights: bfloat16 [256, 32], replicated, may hold values from -0.375 to 0.375
- outer_mixing_weight: bfloat16 [1024, 128], replicated, may hold values from -1 to 1
- widening_weight: bfloat16 [128, 512], replicated, may hold values from -0.5 to 0.5
- narrowing_weight: bfloat16 [512, 128], replicated, may hold values from -0.375 to 0.375
Outputs:
- profile_refreshed: bfloat16 [128, 128, 256], P(('grp', 'gx'), ('gy', 'gz')), parts along dimension 0
- pair_output: bfloat16 [256, 128, 128], P(('grp', 'gy', 'gz'), 'gx'), parts along dimension 0
The draws below stay inside these ranges and needn't reach their ends.
There are 2 independent parts, one for each index of `grp`. The reference program is written for one: setup_inputs(seed, part) draws one part's arguments, and reference() takes and returns one part's arrays. A program takes and returns all parts, laid end to end along the dimension named above; an argument that names none is the same for every part. Nothing has to cross between parts.
All inputs are finite; a program needn't handle non-finite values. No bound on the sum of `alignment_mask` on one device may be relied on, other than what follows from the above.
Results may differ from the reference program's by a relative error of at most 0.013.
Values may be sent and summed in bfloat16 or wider, within the bound.
A program may use at most 64 MiB of HBM per device.

```python
import math
import jax
import jax.numpy as jnp
from jax import lax

PROFILE_DEPTH = 256
HEADS = 8
CZ = 128
PRODUCT_WIDTH = 32
CT = 512
SYMBOL_KINDS = 23
HEAD_DIM = 32
HOMOLOG_NUMBER = 64
CHAIN_LENGTH = 128


def draw_pair_features(key, part):
    values_drawn = jnp.clip(jax.random.normal(jax.random.fold_in(key, 11), (CHAIN_LENGTH, CHAIN_LENGTH, CZ), jnp.float32), -4.0, 4.0)
    return values_drawn.astype(jnp.bfloat16)


def draw_pair_bias_matrix(key, part):
    values_drawn = jnp.clip(0.15 * jax.random.normal(jax.random.fold_in(key, 21), (CZ, HEADS), jnp.float32), -0.9, 0.9)
    return values_drawn


def touch_ends(values, rng, smallest, high):
    dims = values.shape
    spot = [jax.random.randint(jax.random.fold_in(rng, axis), (), 0, dims[axis]) for axis in range(len(dims))]
    values = values.at[tuple(spot)].set(smallest)
    longest = dims.index(max(dims))
    spot[longest] = (spot[longest] + 1) % dims[longest]
    return values.at[tuple(spot)].set(high)


def level_of(stream_key, dims, cuts, low, largest):
    def one(position, blocks):
        draws = jax.random.uniform(jax.random.fold_in(jax.random.fold_in(stream_key, 6), position), (blocks,), jnp.float32, low / len(cuts), largest / len(cuts))
        return jnp.repeat(jnp.exp(draws), dims[position] // blocks).reshape((-1,) + (1,) * (len(dims) - position - 1))

    level = one(*cuts[0])
    for cut in cuts[1:]:
        level = level * one(*cut)
    return level


def gaussian(own_key, extent, scale, most, pieces=(), kind=jnp.bfloat16):
    values = scale * jax.random.normal(own_key, extent, jnp.float32)
    if pieces:
        values = values * level_of(own_key, extent, pieces, -0.22, 0.18)
    return jnp.clip(values, -most, most).astype(kind)


def setup_inputs(seed: int = 0, part: int = 0) -> dict:
    arg_keys = jax.random.split(jax.random.key(seed), 17)
    own_keys = jax.random.split(jax.random.fold_in(arg_keys[16], part), 17)
    return {
        "alignment_token_ids": touch_ends(jax.random.randint(own_keys[0], (HOMOLOG_NUMBER, CHAIN_LENGTH), 0, SYMBOL_KINDS), jax.random.fold_in(own_keys[0], 1), 0, SYMBOL_KINDS - 1).astype(jnp.int32),
        "homolog_profile": gaussian(own_keys[1], (HOMOLOG_NUMBER, CHAIN_LENGTH, PROFILE_DEPTH), 1.0, 6.0, ((0, 4), (1, 4))),
        "alignment_mask": touch_ends((jax.random.randint(own_keys[2], (HOMOLOG_NUMBER, CHAIN_LENGTH), 0, 4) < 3).astype(jnp.int32), jax.random.fold_in(own_keys[2], 1), 0, 1),
        "pair_features": draw_pair_features(jax.random.fold_in(jax.random.fold_in(arg_keys[16], part), 71), part),
        "symbol_lookup_weights": gaussian(arg_keys[4], (SYMBOL_KINDS, PROFILE_DEPTH), 1.0, 6.0),
        "asking_weights": gaussian(arg_keys[5], (PROFILE_DEPTH, PROFILE_DEPTH), PROFILE_DEPTH ** -0.5, 0.375),
        "lookup_weights": gaussian(arg_keys[6], (PROFILE_DEPTH, PROFILE_DEPTH), PROFILE_DEPTH ** -0.5, 0.375),
        "content_weights": gaussian(arg_keys[7], (PROFILE_DEPTH, PROFILE_DEPTH), PROFILE_DEPTH ** -0.5, 0.375),
        "sigmoid_switch_weights": gaussian(arg_keys[8], (PROFILE_DEPTH, PROFILE_DEPTH), PROFILE_DEPTH ** -0.5, 0.375),
        "resulting_weights": gaussian(arg_keys[9], (PROFILE_DEPTH, PROFILE_DEPTH), (PROFILE_DEPTH // 4) ** -0.5, 0.75),
        "pair_bias_matrix": draw_pair_bias_matrix(jax.random.fold_in(arg_keys[16], 71), part),
        "first_factor_weights": gaussian(arg_keys[11], (PROFILE_DEPTH, PRODUCT_WIDTH), PROFILE_DEPTH ** -0.5, 0.375),
        "second_factor_weights": gaussian(arg_keys[12], (PROFILE_DEPTH, PRODUCT_WIDTH), PROFILE_DEPTH ** -0.5, 0.375),
        "outer_mixing_weight": gaussian(arg_keys[13], (PRODUCT_WIDTH * PRODUCT_WIDTH, CZ), PRODUCT_WIDTH ** -0.5, 1.0),
        "widening_weight": gaussian(arg_keys[14], (CZ, CT), CZ ** -0.5, 0.5),
        "narrowing_weight": gaussian(arg_keys[15], (CT, CZ), (CT // 2) ** -0.5, 0.375),
    }


HIGHEST_PRECISION = lax.Precision.HIGHEST

def standardize_lastaxis(values):
    average = lax.optimization_barrier(jnp.mean(values, axis=-1, keepdims=True))
    centred = values - average
    return centred * lax.rsqrt(lax.optimization_barrier(jnp.mean(centred * centred, axis=-1, keepdims=True)) + 1e-05)

def reference(alignment_token_ids, homolog_profile, alignment_mask, pair_features, symbol_lookup_weights, asking_weights, lookup_weights, content_weights, sigmoid_switch_weights, resulting_weights, pair_bias_matrix, first_factor_weights, second_factor_weights, outer_mixing_weight, widening_weight, narrowing_weight):
    profile_arriving = homolog_profile.astype(jnp.float32) + symbol_lookup_weights.astype(jnp.float32)[alignment_token_ids]
    standardized_profile = standardize_lastaxis(profile_arriving).astype(jnp.bfloat16).reshape(HOMOLOG_NUMBER * CHAIN_LENGTH, PROFILE_DEPTH)

    def project(weight):
        return jnp.dot(standardized_profile, weight, preferred_element_type=jnp.float32).astype(jnp.bfloat16).reshape(HOMOLOG_NUMBER, CHAIN_LENGTH, HEADS, HEAD_DIM)
    queries = project(asking_weights)
    keys_all = project(lookup_weights)
    values_all = project(content_weights)
    sigmoid_switch = jax.nn.sigmoid(jnp.dot(standardized_profile, sigmoid_switch_weights, preferred_element_type=jnp.float32)).reshape(HOMOLOG_NUMBER, CHAIN_LENGTH, PROFILE_DEPTH)
    pair_bias = jnp.einsum('ijc,ch->ihj', standardize_lastaxis(pair_features.astype(jnp.float32)), pair_bias_matrix, precision=HIGHEST_PRECISION)
    mask_penalty = (alignment_mask.astype(jnp.float32) - 1.0) * 1000000000.0

    def row_attention(row_parts):
        query_row, key_row, value_row, penalty_row = row_parts
        scores = jnp.einsum('ihd,jhd->ihj', query_row.astype(jnp.float32), key_row.astype(jnp.float32), precision=HIGHEST_PRECISION) * HEAD_DIM ** (-0.5)
        scores = scores + pair_bias + penalty_row[None, None, :]
        top = lax.optimization_barrier(jnp.max(scores, axis=-1, keepdims=True))
        exp_scores = jnp.exp(scores - top)
        aggregate = lax.optimization_barrier(jnp.sum(exp_scores, axis=-1))
        weights = exp_scores.astype(jnp.bfloat16)
        accumulated = jnp.einsum('ihj,jhd->ihd', weights.astype(jnp.float32), value_row.astype(jnp.float32), precision=HIGHEST_PRECISION)
        return (accumulated / aggregate[:, :, None]).reshape(CHAIN_LENGTH, PROFILE_DEPTH)
    softmax_combined = lax.map(row_attention, (queries, keys_all, values_all, mask_penalty))
    switched_result = (sigmoid_switch * softmax_combined).astype(jnp.bfloat16).reshape(HOMOLOG_NUMBER * CHAIN_LENGTH, PROFILE_DEPTH)
    profile_refreshed = (profile_arriving + jnp.dot(switched_result, resulting_weights, preferred_element_type=jnp.float32).reshape(HOMOLOG_NUMBER, CHAIN_LENGTH, PROFILE_DEPTH)).astype(jnp.bfloat16)
    averaged_products = standardize_lastaxis(profile_refreshed.astype(jnp.float32)).astype(jnp.bfloat16).reshape(HOMOLOG_NUMBER * CHAIN_LENGTH, PROFILE_DEPTH)
    mask_floating = alignment_mask.astype(jnp.float32)
    left_side = (jnp.dot(averaged_products, first_factor_weights, preferred_element_type=jnp.float32).reshape(HOMOLOG_NUMBER, CHAIN_LENGTH, PRODUCT_WIDTH) * mask_floating[:, :, None]).astype(jnp.bfloat16).reshape(HOMOLOG_NUMBER, CHAIN_LENGTH * PRODUCT_WIDTH)
    right_side = (jnp.dot(averaged_products, second_factor_weights, preferred_element_type=jnp.float32).reshape(HOMOLOG_NUMBER, CHAIN_LENGTH, PRODUCT_WIDTH) * mask_floating[:, :, None]).astype(jnp.bfloat16).reshape(HOMOLOG_NUMBER, CHAIN_LENGTH * PRODUCT_WIDTH)
    pair_count = jnp.dot(mask_floating.T, mask_floating, precision=HIGHEST_PRECISION)
    panel_rows = math.gcd(CHAIN_LENGTH, 16)

    def outer_panel(panel_index):
        left_rows = lax.dynamic_slice_in_dim(left_side, panel_index * (panel_rows * PRODUCT_WIDTH), panel_rows * PRODUCT_WIDTH, 1)
        outer_block = jnp.dot(left_rows.T, right_side, preferred_element_type=jnp.float32).astype(jnp.bfloat16)
        outer_block = outer_block.reshape(panel_rows, PRODUCT_WIDTH, CHAIN_LENGTH, PRODUCT_WIDTH).transpose(0, 2, 1, 3).reshape(panel_rows * CHAIN_LENGTH, PRODUCT_WIDTH * PRODUCT_WIDTH)
        return jnp.dot(outer_block, outer_mixing_weight, preferred_element_type=jnp.float32).reshape(panel_rows, CHAIN_LENGTH, CZ)
    mixed_pair = lax.map(outer_panel, jnp.arange(CHAIN_LENGTH // panel_rows, dtype=jnp.int32)).reshape(CHAIN_LENGTH, CHAIN_LENGTH, CZ)
    pair_mid = pair_features.astype(jnp.float32) + mixed_pair / (pair_count[:, :, None] + 1.0)
    trans_rows = standardize_lastaxis(pair_mid).astype(jnp.bfloat16).reshape(CHAIN_LENGTH * CHAIN_LENGTH, CZ)
    expanded = jax.nn.relu(jnp.dot(trans_rows, widening_weight, preferred_element_type=jnp.float32)).astype(jnp.bfloat16)
    pair_output = (pair_mid + jnp.dot(expanded, narrowing_weight, preferred_element_type=jnp.float32).reshape(CHAIN_LENGTH, CHAIN_LENGTH, CZ)).astype(jnp.bfloat16)
    return (profile_refreshed, pair_output)
```

```python
import functools

import jax
import jax.numpy as jnp
from jax import lax
from jax.experimental import pallas as pl
from jax.experimental.pallas import tpu as pltpu
from jax.sharding import PartitionSpec as P

MESH = pl.DeviceIdType.MESH
F32, BF16 = jnp.float32, jnp.bfloat16


def standardize(values):
    average = jnp.mean(values, axis=-1, keepdims=True)
    centred = values - average
    return centred * lax.rsqrt(jnp.mean(centred * centred, axis=-1, keepdims=True) + 1e-05)


def contract(a, b, dim_a, dim_b, precision=None):
    return lax.dot_general(
        a, b, (((dim_a,), (dim_b,)), ((), ())), precision=precision, preferred_element_type=F32
    )


def kernel(
    sizes,
    ids, hp, mask, pf, tab, wq, wk, wv, wg, wo, wb, w1, w2, wm, ww, wn,
    prof_out, pair_out,
    xg, idg, mg, mx, mc, bx, lg, zs, zr,
    ida, pen, bias, xown, qown, gown, lf, zf, lmask, wt, wf, rbd, osc,
    hy_s, hy_r, hz_s, hz_r, ig_s, ig_r, mg_s, mg_r, mx_s, mx_r, mc_s, mc_r,
    bx_s, bx_r, lg_s, lg_r, zr_s, zr_r, lc_s,
):
    nx, ny, nz, chunk = sizes
    nr = ny * nz
    seqs, res, depth = hp.shape
    heads = wb.shape[1]
    hd = depth // heads
    side = w1.shape[1]
    zdim = pf.shape[2]
    kinds = tab.shape[0]
    keys = nr * res
    pack = zdim // res
    grp = res // pack
    chunks = seqs // chunk
    q = lax.axis_index("gx")
    y = lax.axis_index("gy")
    z = lax.axis_index("gz")
    r = y * nz + z

    def at_r(index):
        return {"gy": index // nz, "gz": index % nz}

    barrier = pltpu.get_barrier_semaphore()
    for k in range(1, nr):
        pl.semaphore_signal(barrier, inc=1, device_id=at_r((r + k) % nr), device_id_type=MESH)
    for k in range(1, nx):
        pl.semaphore_signal(barrier, inc=1, device_id={"gx": (q + k) % nx}, device_id_type=MESH)
    for k in range(nx):
        @pl.when(jnp.logical_or(q != k, r != q))
        def _():
            pl.semaphore_signal(
                barrier, inc=1, device_id={"gx": k, **at_r(q)}, device_id_type=MESH
            )
    diagonal = jnp.where(q == r, 1, 0)
    pl.semaphore_wait(barrier, (nr - 1) + (nx - 1) + nr - diagonal)

    def remote(src, dst, send, recv, device):
        return pltpu.make_async_remote_copy(
            src_ref=src, dst_ref=dst, send_sem=send, recv_sem=recv,
            device_id=device, device_id_type=MESH,
        )

    def hy(k, c):
        part = pl.ds(c * chunk, chunk)
        return remote(
            hp.at[part], xg.at[r, part], hy_s.at[k - 1, c], hy_r.at[k - 1, c],
            {"gy": (y + k) % ny},
        )

    def hz(k, m, c):
        part = pl.ds(c * chunk, chunk)
        slot = ((y + ny - k) % ny) * nz + z
        src = hp.at[part] if k == 0 else xg.at[slot, part]
        return remote(
            src, xg.at[slot, part], hz_s.at[k, m - 1, c], hz_r.at[k, m - 1, c],
            {"gz": (z + m) % nz},
        )

    def ig(k):
        return remote(ids, idg.at[r], ig_s.at[k - 1], ig_r.at[k - 1], at_r((r + k) % nr))

    def mgc(k):
        return remote(mask, mg.at[r], mg_s.at[k - 1], mg_r.at[k - 1], at_r((r + k) % nr))

    def gxc(buffer, send, recv, k):
        return remote(
            buffer.at[q], buffer.at[q], send.at[k - 1], recv.at[k - 1], {"gx": (q + k) % nx}
        )

    def crossing(src, buffer, send, recv, k):
        return remote(src, buffer.at[q], send.at[k], recv.at[q], {"gx": r, **at_r(k)})

    def crossing_wait(src, buffer, send, recv, k):
        return remote(src, buffer.at[k], send.at[0], recv.at[k], {"gx": k, **at_r(q)})

    for c in range(chunks):
        for k in range(1, ny):
            hy(k, c).start()
    for k in range(1, nr):
        ig(k).start()
        mgc(k).start()
    for c in range(chunks):
        for m in range(1, nz):
            hz(0, m, c).start()
    own = pltpu.make_async_copy(hp, xg.at[r], lc_s)
    own.start()
    mx[q] = mask[...]
    for k in range(1, nx):
        remote(mask, mx.at[q], mx_s.at[k - 1], mx_r.at[k - 1], {"gx": (q + k) % nx}).start()
    for k in range(nr):
        @pl.when(jnp.logical_or(q != r, r != k))
        def _():
            crossing(mask, mc, mc_s, mc_r, k).start()

    @pl.when(q == r)
    def _():
        mc[q] = mask[...]

    pair_rows = pf[...].astype(F32).reshape(res * res, zdim)
    bx[q] = contract(wb[...], standardize(pair_rows), 0, 1, lax.Precision.HIGHEST)
    for k in range(1, nx):
        gxc(bx, bx_s, bx_r, k).start()

    label = lax.broadcasted_iota(jnp.int32, (kinds, res), 0)
    table = tab[...]
    for s in range(seqs):
        hot = jnp.where(label == ids[s : s + 1, :], 1.0, 0.0).astype(BF16)
        xown[s * res : (s + 1) * res, :] = hp[s].astype(F32) + contract(hot, table, 0, 0)
    normed = standardize(xown[...]).astype(BF16)
    qown[...] = jnp.dot(normed, wq[...], preferred_element_type=F32).astype(BF16)
    gown[...] = jax.nn.sigmoid(jnp.dot(normed, wg[...], preferred_element_type=F32))

    wf[...] = wm[...].astype(F32)
    for d in range(side):
        wt[:, d * side : (d + 1) * side] = wf[pl.ds(d, side, stride=side), :].T.astype(BF16)

    spread = jnp.where(
        lax.broadcasted_iota(jnp.int32, (grp, grp * side), 0)
        == lax.broadcasted_iota(jnp.int32, (grp, grp * side), 1) // side,
        1.0, 0.0,
    ).astype(BF16)
    maskf = mask[...].astype(F32)
    for p in range(pack):
        lmask[p * seqs : (p + 1) * seqs, :] = jnp.dot(
            maskf[:, p * grp : (p + 1) * grp].astype(BF16), spread, preferred_element_type=F32
        )
    mask4 = jnp.concatenate([maskf] * pack, axis=1)

    idg[r] = ids[...]
    mg[r] = mask[...]
    for k in range(1, nr):
        ig(k).wait_recv()
        mgc(k).wait_recv()
    ida[...] = jnp.concatenate([idg[k] for k in range(nr)], axis=1)
    pen[...] = (
        jnp.concatenate([mg[k] for k in range(nr)], axis=1).astype(F32) - 1.0
    ) * 1000000000.0

    for k in range(1, nx):
        remote(mask, mx.at[q], mx_s.at[k - 1], mx_r.at[k - 1], {"gx": (q + k) % nx}).wait_recv()
    for k in range(nx):
        @pl.when(jnp.logical_or(q != r, q != k))
        def _():
            crossing_wait(mask, mc, mc_s, mc_r, k).wait_recv()
    count = contract(
        mx[...].reshape(nx * seqs, res).astype(F32), mc[...].reshape(nx * seqs, res).astype(F32), 0, 0
    )
    share = 1.0 / (
        jnp.concatenate([count[p * grp : (p + 1) * grp, :] for p in range(pack)], axis=1) + 1.0
    )

    for k in range(1, nx):
        gxc(bx, bx_s, bx_r, k).wait_recv()
    for i in range(res):
        bias[:, i, :] = jnp.concatenate(
            [bx[k, :, i * res : (i + 1) * res] for k in range(nx)], axis=1
        )
    own.wait()

    scale = hd ** (-0.5)
    label_all = lax.broadcasted_iota(jnp.int32, (kinds, keys), 0)
    lane_head = lax.broadcasted_iota(jnp.int32, (res, depth), 1) // hd
    lane_block = lax.broadcasted_iota(jnp.int32, (seqs, zdim), 1) // res
    lane_block8 = lax.broadcasted_iota(jnp.int32, (side // pack, zdim), 1) // res
    w1x = jnp.concatenate([w1[...]] * pack, axis=1)

    def step(c, carry):
        for k in range(1, ny):
            hy(k, c).wait_recv()
            for m in range(1, nz):
                hz(k, m, c).start()
        for k in range(ny):
            for m in range(1, nz):
                hz(k, m, c).wait_recv()
        first = c * chunk
        normed_rows = []
        for t in range(chunk):
            hot = jnp.where(label_all == ida[pl.ds(first + t, 1), :], 1.0, 0.0).astype(BF16)
            rows = jnp.concatenate([xg[k, first + t] for k in range(nr)], axis=0).astype(F32)
            normed_rows.append(standardize(rows + contract(hot, table, 0, 0)).astype(BF16))
        normed_rows = jnp.concatenate(normed_rows, axis=0)
        key_rows = jnp.dot(normed_rows, wk[...], preferred_element_type=F32).astype(BF16)
        value_rows = jnp.dot(normed_rows, wv[...], preferred_element_type=F32).astype(BF16)
        bias_rows = bias[...].reshape(heads * res, keys)
        attended = []
        for t in range(chunk):
            base = pl.multiple_of((first + t) * res, res)
            query = qown[pl.ds(base, res), :]
            spread_query = jnp.concatenate(
                [jnp.where(lane_head == h, query, jnp.zeros_like(query)) for h in range(heads)],
                axis=0,
            )
            scores = contract(spread_query, key_rows[t * keys : (t + 1) * keys], 1, 1) * scale
            scores = scores + bias_rows + pen[pl.ds(first + t, 1), :]
            top = jnp.max(scores, axis=-1, keepdims=True)
            weights = jnp.exp(scores - top)
            total = jnp.sum(weights, axis=-1, keepdims=True)
            mixed = jnp.dot(
                weights.astype(BF16), value_rows[t * keys : (t + 1) * keys],
                preferred_element_type=F32,
            ) * (1.0 / total)
            picked = mixed[0:res]
            for h in range(1, heads):
                picked = jnp.where(lane_head == h, mixed[h * res : (h + 1) * res], picked)
            attended.append((gown[pl.ds(base, res), :] * picked).astype(BF16))
        base = pl.multiple_of(first * res, chunk * res)
        refreshed = (
            xown[pl.ds(base, chunk * res), :]
            + jnp.dot(jnp.concatenate(attended, axis=0), wo[...], preferred_element_type=F32)
        ).astype(BF16)
        prof_out[pl.ds(first, chunk)] = refreshed.reshape(chunk, res, depth)
        opm = standardize(refreshed.astype(F32)).astype(BF16)
        lf[pl.ds(base, chunk * res), :] = jnp.dot(opm, w1x, preferred_element_type=F32)
        right = contract(w2[...], opm, 0, 1)
        eighth = side // pack
        for t in range(chunk):
            tile = None
            for p in range(pack):
                shift = ((p - t) * res) % (chunk * res)
                piece = right[p * eighth : (p + 1) * eighth, :]
                piece = pltpu.roll(piece, shift, 1) if shift else piece
                tile = piece if tile is None else jnp.where(lane_block8 == p, piece, tile)
            zf[:, pl.ds(first + t, 1), :] = tile[:, None, :]
        return carry

    lax.fori_loop(0, chunks, step, 0)

    for p in range(pack):
        for half in range(grp // pack):
            tile = None
            for b in range(pack):
                piece = lf[pl.ds(p * grp + half * pack + b, seqs, stride=res), :]
                tile = piece if tile is None else jnp.where(lane_block == b, piece, tile)
            rows, lanes = slice(p * seqs, (p + 1) * seqs), slice(half * zdim, (half + 1) * zdim)
            lg[q, rows, lanes] = (tile * lmask[rows, lanes]).astype(BF16)
    for k in range(1, nx):
        gxc(lg, lg_s, lg_r, k).start()
    zs[...] = (zf[...] * mask4[None]).astype(BF16)
    for k in range(nr):
        @pl.when(jnp.logical_or(q != r, r != k))
        def _():
            crossing(zs, zr, zr_s, zr_r, k).start()

    @pl.when(q == r)
    def _():
        zr[q] = zs[...]

    eighth = side // pack
    place_row = lax.broadcasted_iota(jnp.int32, (zdim, pack * zdim), 0)
    place_col = lax.broadcasted_iota(jnp.int32, (zdim, pack * zdim), 1)
    placing = jnp.where(
        (place_row // res == place_col // zdim) & (place_row % res == place_col % res), 1.0, 0.0
    ).astype(BF16)
    for k in range(nx):
        @pl.when(jnp.logical_or(q != r, q != k))
        def _():
            crossing_wait(zs, zr, zr_s, zr_r, k).wait_recv()
    for k in range(nx):
        wide = jnp.dot(
            zr[k].reshape(eighth * seqs, zdim), placing, preferred_element_type=F32
        ).astype(BF16)
        for e in range(eighth):
            for p in range(pack):
                piece = wide[e * seqs : (e + 1) * seqs, p * zdim : (p + 1) * zdim]
                d = p * eighth + e
                for b in range(pack):
                    row = (k * pack + b) * seqs
                    rbd[row : row + seqs, d * zdim : (d + 1) * zdim] = jnp.where(
                        lane_block == b, piece, jnp.zeros_like(piece)
                    )
    for k in range(1, nx):
        gxc(lg, lg_s, lg_r, k).wait_recv()
    left = lg[...].reshape(nx * pack * seqs, grp * side)
    for e in range(eighth):
        cols = slice(e * pack * zdim, (e + 1) * pack * zdim)
        product = contract(left, rbd[:, cols], 0, 0).astype(BF16)
        for p in range(pack):
            d = e * pack + p
            for g in range(grp):
                osc[d * side : (d + 1) * side, g * zdim : (g + 1) * zdim] = product[
                    g * side : (g + 1) * side, p * zdim : (p + 1) * zdim
                ]
    for g in range(0, grp, 2):
        both = jnp.dot(
            wt[...], osc[:, g * zdim : (g + 2) * zdim], preferred_element_type=F32
        )
        middle = []
        for u in range(2):
            part = both[:, u * zdim : (u + 1) * zdim] * share[g + u : g + u + 1, :]
            pair_g = jnp.concatenate([pf[p * grp + g + u] for p in range(pack)], axis=0)
            middle.append(pair_g.astype(F32) + part.T)
        middle = jnp.concatenate(middle, axis=0)
        trans = standardize(middle).astype(BF16)
        expanded = jnp.maximum(
            jnp.dot(trans, ww[...], preferred_element_type=F32), 0.0
        ).astype(BF16)
        result = (middle + jnp.dot(expanded, wn[...], preferred_element_type=F32)).astype(BF16)
        for u in range(2):
            for p in range(pack):
                start = u * zdim + p * res
                pair_out[p * grp + g + u] = result[start : start + res]

    for c in range(chunks):
        for k in range(1, ny):
            hy(k, c).wait_send()
        for k in range(ny):
            for m in range(1, nz):
                hz(k, m, c).wait_send()
    for k in range(1, nr):
        ig(k).wait_send()
        mgc(k).wait_send()
    for k in range(1, nx):
        remote(mask, mx.at[q], mx_s.at[k - 1], mx_r.at[k - 1], {"gx": (q + k) % nx}).wait_send()
        gxc(bx, bx_s, bx_r, k).wait_send()
        gxc(lg, lg_s, lg_r, k).wait_send()
    for k in range(nr):
        @pl.when(jnp.logical_or(q != r, r != k))
        def _():
            crossing(mask, mc, mc_s, mc_r, k).wait_send()
            crossing(zs, zr, zr_s, zr_r, k).wait_send()


def solution(mesh):
    nx, ny, nz = mesh.shape["gx"], mesh.shape["gy"], mesh.shape["gz"]
    nr = ny * nz

    def local(*arrays):
        hp, pf, wb, w1, wm = arrays[1], arrays[3], arrays[10], arrays[11], arrays[13]
        seqs, res, depth = hp.shape
        zdim = pf.shape[2]
        heads, side = wb.shape[1], w1.shape[1]
        keys, pack = nr * res, zdim // res
        grp = res // pack
        chunk = pack
        chunks = seqs // chunk
        dma = pltpu.SemaphoreType.DMA
        vm = pltpu.VMEM
        scratch = [
            vm((nr, seqs, res, depth), BF16),
            vm((nr, seqs, res), jnp.int32),
            vm((nr, seqs, res), jnp.int32),
            vm((nx, seqs, res), jnp.int32),
            vm((nx, seqs, res), jnp.int32),
            vm((nx, heads, res * res), F32),
            vm((nx, pack * seqs, grp * side), BF16),
            vm((side // pack, seqs, zdim), BF16),
            vm((nx, side // pack, seqs, zdim), BF16),
            vm((seqs, keys), jnp.int32),
            vm((seqs, keys), F32),
            vm((heads, res, keys), F32),
            vm((seqs * res, depth), F32),
            vm((seqs * res, depth), BF16),
            vm((seqs * res, depth), F32),
            vm((seqs * res, zdim), F32),
            vm((side // pack, seqs, zdim), F32),
            vm((pack * seqs, grp * side), F32),
            vm((zdim, side * side), BF16),
            vm(wm.shape, F32),
            vm((nx * pack * seqs, side * zdim), BF16),
            vm((side * side, res * res), BF16),
            dma((max(ny - 1, 1), chunks)), dma((max(ny - 1, 1), chunks)),
            dma((ny, max(nz - 1, 1), chunks)), dma((ny, max(nz - 1, 1), chunks)),
            dma((nr,)), dma((nr,)), dma((nr,)), dma((nr,)),
            dma((nx,)), dma((nx,)), dma((nr,)), dma((nx,)),
            dma((nx,)), dma((nx,)), dma((nx,)), dma((nx,)),
            dma((nr,)), dma((nx,)), dma,
        ]
        return pl.pallas_call(
            functools.partial(kernel, (nx, ny, nz, chunk)),
            out_shape=(
                jax.ShapeDtypeStruct(hp.shape, BF16),
                jax.ShapeDtypeStruct(pf.shape, BF16),
            ),
            in_specs=[pl.BlockSpec(memory_space=pltpu.VMEM)] * len(arrays),
            out_specs=(pl.BlockSpec(memory_space=pltpu.VMEM),) * 2,
            scratch_shapes=scratch,
            compiler_params=pltpu.CompilerParams(
                collective_id=0, has_side_effects=True, vmem_limit_bytes=60 * 1024 * 1024
            ),
        )(*arrays)

    in_specs = (
        P(("grp", "gx"), ("gy", "gz")),
        P(("grp", "gx"), ("gy", "gz"), None),
        P(("grp", "gx"), ("gy", "gz")),
        P(("grp", "gy", "gz"), "gx", None),
    ) + (P(),) * 12
    out_specs = (P(("grp", "gx"), ("gy", "gz"), None), P(("grp", "gy", "gz"), "gx", None))
    return jax.shard_map(local, mesh=mesh, in_specs=in_specs, out_specs=out_specs, check_vma=False)
```

```python
import functools

import jax
import jax.numpy as jnp
from jax import lax
from jax.experimental import pallas as pl
from jax.experimental.pallas import tpu as pltpu
from jax.sharding import PartitionSpec as P

MESH = pl.DeviceIdType.MESH
LATE = (3, 5, 6, 7, 8, 9, 13, 14, 15)
F32, BF16 = jnp.float32, jnp.bfloat16


def standardize(values):
    average = jnp.mean(values, axis=-1, keepdims=True)
    centred = values - average
    return centred * lax.rsqrt(jnp.mean(centred * centred, axis=-1, keepdims=True) + 1e-05)


def contract(a, b, dim_a, dim_b, precision=None):
    return lax.dot_general(
        a, b, (((dim_a,), (dim_b,)), ((), ())), precision=precision, preferred_element_type=F32
    )


def kernel(
    sizes,
    ids, hp, mask, hf, tab, hq, hk, hv, hg, ho, wb, w1, w2, hm, hw, hn,
    prof_out, pair_out,
    xg, idg, mg, mx, mc, bx, lg, zs, zr,
    ida, pen, bias, xown, qown, gown, lf, zf, lmask, wt, wf, rbd, osc,
    hy_s, hy_r, hz_s, hz_r, ig_s, ig_r, mg_s, mg_r, mx_s, mx_r, mc_s, mc_r,
    bx_s, bx_r, lg_s, lg_r, zr_s, zr_r, lc_s, sw_s, sw_r,
    vf, vq, vk, vv, vg, vo, vm_, vw, vn, load_s,
):
    nx, ny, nz, chunk = sizes
    pf, wq, wk, wv, wg, wo, wm, ww, wn = vf, vq, vk, vv, vg, vo, vm_, vw, vn
    far = (hf, hq, hk, hv, hg, ho, hm, hw, hn)
    near = (pf, wq, wk, wv, wg, wo, wm, ww, wn)
    loads = [pltpu.make_async_copy(a, b, load_s.at[k]) for k, (a, b) in enumerate(zip(far, near))]
    nr = ny * nz
    seqs, res, depth = hp.shape
    heads = wb.shape[0]
    hd = depth // heads
    side = w1.shape[0]
    zdim = pf.shape[2]
    kinds = tab.shape[0]
    keys = nr * res
    pack = zdim // res
    grp = res // pack
    chunks = seqs // chunk
    q = lax.axis_index("gx")
    y = lax.axis_index("gy")
    z = lax.axis_index("gz")
    r = y * nz + z

    def at_r(index):
        return {"gy": index // nz, "gz": index % nz}

    barrier = pltpu.get_barrier_semaphore()
    for k in range(1, nr):
        pl.semaphore_signal(barrier, inc=1, device_id=at_r((r + k) % nr), device_id_type=MESH)
    for k in range(1, nx):
        pl.semaphore_signal(barrier, inc=1, device_id={"gx": (q + k) % nx}, device_id_type=MESH)
    for k in range(nx):
        @pl.when(jnp.logical_or(q != k, r != q))
        def _():
            pl.semaphore_signal(
                barrier, inc=1, device_id={"gx": k, **at_r(q)}, device_id_type=MESH
            )
    for load in loads:
        load.start()
    diagonal = jnp.where(q == r, 1, 0)
    pl.semaphore_wait(barrier, (nr - 1) + (nx - 1) + nr - diagonal)

    def remote(src, dst, send, recv, device):
        return pltpu.make_async_remote_copy(
            src_ref=src, dst_ref=dst, send_sem=send, recv_sem=recv,
            device_id=device, device_id_type=MESH,
        )

    def hy(k, c):
        part = pl.ds(c * chunk, chunk)
        return remote(
            hp.at[part], xg.at[r, part], hy_s.at[k - 1, c], hy_r.at[k - 1, c],
            {"gy": (y + k) % ny},
        )

    def hz(k, m, c):
        part = pl.ds(c * chunk, chunk)
        slot = ((y + ny - k) % ny) * nz + z
        src = hp.at[part] if k == 0 else xg.at[slot, part]
        return remote(
            src, xg.at[slot, part], hz_s.at[k, m - 1, c], hz_r.at[k, m - 1, c],
            {"gz": (z + m) % nz},
        )

    def ig(k):
        return remote(ids, idg.at[r], ig_s.at[k - 1], ig_r.at[k - 1], at_r((r + k) % nr))

    def mgc(k):
        return remote(mask, mg.at[r], mg_s.at[k - 1], mg_r.at[k - 1], at_r((r + k) % nr))

    def gxc(buffer, send, recv, k):
        return remote(
            buffer.at[q], buffer.at[q], send.at[k - 1], recv.at[k - 1], {"gx": (q + k) % nx}
        )

    def crossing(src, buffer, send, recv, k):
        return remote(src, buffer.at[q], send.at[k], recv.at[q], {"gx": r, **at_r(k)})

    def swap():
        return remote(zs, zr.at[q], sw_s, sw_r, {"gx": r, **at_r(q)})

    def swap_wait():
        return remote(zs, zr.at[r], sw_s, sw_r, {"gx": r, **at_r(q)})

    def spread_right(k):
        return remote(
            zr.at[r], zr.at[r], zr_s.at[k - 1], zr_r.at[k - 1], at_r((r + k) % nr)
        )

    def crossing_wait(src, buffer, send, recv, k):
        return remote(src, buffer.at[k], send.at[0], recv.at[k], {"gx": k, **at_r(q)})

    for k in range(1, nr):
        ig(k).start()
        mgc(k).start()
    mx[q] = mask[...]
    for k in range(1, nx):
        remote(mask, mx.at[q], mx_s.at[k - 1], mx_r.at[k - 1], {"gx": (q + k) % nx}).start()
    for k in range(nr):
        @pl.when(jnp.logical_or(q != r, r != k))
        def _():
            crossing(mask, mc, mc_s, mc_r, k).start()

    @pl.when(q == r)
    def _():
        mc[q] = mask[...]

    for c in range(chunks):
        for k in range(1, ny):
            hy(k, c).start()
    for c in range(chunks):
        for m in range(1, nz):
            hz(0, m, c).start()
    own = pltpu.make_async_copy(hp, xg.at[r], lc_s)
    own.start()

    loads[0].wait()
    pair_rows = pf[...].astype(F32).reshape(res * res, zdim)
    bx[q] = contract(wb[...], standardize(pair_rows), 1, 1, lax.Precision.HIGHEST)
    for k in range(1, nx):
        gxc(bx, bx_s, bx_r, k).start()

    label = lax.broadcasted_iota(jnp.int32, (kinds, res), 0)
    table = tab[...]
    for s in range(seqs):
        hot = jnp.where(label == ids[s : s + 1, :], 1.0, 0.0).astype(BF16)
        xown[s * res : (s + 1) * res, :] = hp[s].astype(F32) + contract(hot, table, 0, 0)
    normed = standardize(xown[...]).astype(BF16)
    for load in loads[1:]:
        load.wait()
    qown[...] = jnp.dot(normed, wq[...], preferred_element_type=F32).astype(BF16)
    gown[...] = jax.nn.sigmoid(jnp.dot(normed, wg[...], preferred_element_type=F32))

    wf[...] = wm[...].astype(F32)
    for d in range(side):
        wt[:, d * side : (d + 1) * side] = wf[pl.ds(d, side, stride=side), :].T.astype(BF16)

    spread = jnp.where(
        lax.broadcasted_iota(jnp.int32, (grp, grp * side), 0)
        == lax.broadcasted_iota(jnp.int32, (grp, grp * side), 1) // side,
        1.0, 0.0,
    ).astype(BF16)
    maskf = mask[...].astype(F32)
    for p in range(pack):
        lmask[p * seqs : (p + 1) * seqs, :] = jnp.dot(
            maskf[:, p * grp : (p + 1) * grp].astype(BF16), spread, preferred_element_type=F32
        )
    mask4 = jnp.concatenate([maskf] * pack, axis=1)

    idg[r] = ids[...]
    mg[r] = mask[...]
    for k in range(1, nr):
        ig(k).wait_recv()
        mgc(k).wait_recv()
    ida[...] = jnp.concatenate([idg[k] for k in range(nr)], axis=1)
    pen[...] = (
        jnp.concatenate([mg[k] for k in range(nr)], axis=1).astype(F32) - 1.0
    ) * 1000000000.0

    for k in range(1, nx):
        remote(mask, mx.at[q], mx_s.at[k - 1], mx_r.at[k - 1], {"gx": (q + k) % nx}).wait_recv()
    for k in range(nx):
        @pl.when(jnp.logical_or(q != r, q != k))
        def _():
            crossing_wait(mask, mc, mc_s, mc_r, k).wait_recv()
    count = contract(
        mx[...].reshape(nx * seqs, res).astype(F32), mc[...].reshape(nx * seqs, res).astype(F32), 0, 0
    )
    share = 1.0 / (
        jnp.concatenate([count[p * grp : (p + 1) * grp, :] for p in range(pack)], axis=1) + 1.0
    )

    for k in range(1, nx):
        gxc(bx, bx_s, bx_r, k).wait_recv()
    for i in range(res):
        bias[:, i, :] = jnp.concatenate(
            [bx[k, :, i * res : (i + 1) * res] for k in range(nx)], axis=1
        )
    own.wait()

    scale = hd ** (-0.5)
    label_all = lax.broadcasted_iota(jnp.int32, (kinds, keys), 0)
    lane_head = lax.broadcasted_iota(jnp.int32, (res, depth), 1) // hd
    lane_block = lax.broadcasted_iota(jnp.int32, (seqs, zdim), 1) // res
    lane_block8 = lax.broadcasted_iota(jnp.int32, (side // pack, zdim), 1) // res
    w1x = jnp.concatenate([w1[...]] * pack, axis=0)

    def pass_on(c):
        for k in range(1, ny):
            hy(k, c).wait_recv()
            for m in range(1, nz):
                hz(k, m, c).start()

    pass_on(0)

    def step(c, carry):
        for k in range(ny):
            for m in range(1, nz):
                hz(k, m, c).wait_recv()
        first = c * chunk
        normed_rows = []
        for t in range(chunk):
            hot = jnp.where(label_all == ida[pl.ds(first + t, 1), :], 1.0, 0.0).astype(BF16)
            rows = jnp.concatenate([xg[k, first + t] for k in range(nr)], axis=0).astype(F32)
            normed_rows.append(standardize(rows + contract(hot, table, 0, 0)).astype(BF16))
        normed_rows = jnp.concatenate(normed_rows, axis=0)
        key_rows = jnp.dot(normed_rows, wk[...], preferred_element_type=F32).astype(BF16)
        value_rows = jnp.dot(normed_rows, wv[...], preferred_element_type=F32).astype(BF16)
        bias_rows = bias[...].reshape(heads * res, keys)
        attended = []
        for t in range(chunk):
            base = pl.multiple_of((first + t) * res, res)
            query = qown[pl.ds(base, res), :]
            spread_query = jnp.concatenate(
                [jnp.where(lane_head == h, query, jnp.zeros_like(query)) for h in range(heads)],
                axis=0,
            )
            scores = contract(spread_query, key_rows[t * keys : (t + 1) * keys], 1, 1) * scale
            scores = scores + bias_rows + pen[pl.ds(first + t, 1), :]
            top = jnp.max(scores, axis=-1, keepdims=True)
            weights = jnp.exp(scores - top)
            total = jnp.sum(weights, axis=-1, keepdims=True)
            mixed = jnp.dot(
                weights.astype(BF16), value_rows[t * keys : (t + 1) * keys],
                preferred_element_type=F32,
            ) * (1.0 / total)
            picked = mixed[0:res]
            for h in range(1, heads):
                picked = jnp.where(lane_head == h, mixed[h * res : (h + 1) * res], picked)
            attended.append((gown[pl.ds(base, res), :] * picked).astype(BF16))
        @pl.when(c + 1 < chunks)
        def _():
            pass_on(c + 1)

        base = pl.multiple_of(first * res, chunk * res)
        refreshed = (
            xown[pl.ds(base, chunk * res), :]
            + jnp.dot(jnp.concatenate(attended, axis=0), wo[...], preferred_element_type=F32)
        ).astype(BF16)
        prof_out[pl.ds(first, chunk)] = refreshed.reshape(chunk, res, depth)
        opm = standardize(refreshed.astype(F32)).astype(BF16)
        lf[pl.ds(base, chunk * res), :] = contract(opm, w1x, 1, 1)
        right = contract(w2[...], opm, 1, 1)
        eighth = side // pack
        for t in range(chunk):
            tile = None
            for p in range(pack):
                shift = ((p - t) * res) % (chunk * res)
                piece = right[p * eighth : (p + 1) * eighth, :]
                piece = pltpu.roll(piece, shift, 1) if shift else piece
                tile = piece if tile is None else jnp.where(lane_block8 == p, piece, tile)
            zf[:, pl.ds(first + t, 1), :] = tile[:, None, :]
        return carry

    lax.fori_loop(0, chunks, step, 0)

    zs[...] = (zf[...] * mask4[None]).astype(BF16)
    @pl.when(q != r)
    def _():
        swap().start()

    for p in range(pack):
        for half in range(grp // pack):
            tile = None
            for b in range(pack):
                piece = lf[pl.ds(p * grp + half * pack + b, seqs, stride=res), :]
                tile = piece if tile is None else jnp.where(lane_block == b, piece, tile)
            rows, lanes = slice(p * seqs, (p + 1) * seqs), slice(half * zdim, (half + 1) * zdim)
            lg[q, rows, lanes] = (tile * lmask[rows, lanes]).astype(BF16)
    for k in range(1, nx):
        gxc(lg, lg_s, lg_r, k).start()
    @pl.when(q == r)
    def _():
        zr[q] = zs[...]

    @pl.when(q != r)
    def _():
        swap_wait().wait_recv()

    for k in range(1, nr):
        spread_right(k).start()

    eighth = side // pack
    place_row = lax.broadcasted_iota(jnp.int32, (zdim, pack * zdim), 0)
    place_col = lax.broadcasted_iota(jnp.int32, (zdim, pack * zdim), 1)
    placing = jnp.where(
        (place_row // res == place_col // zdim) & (place_row % res == place_col % res), 1.0, 0.0
    ).astype(BF16)
    for k in range(1, nr):
        spread_right(k).wait_recv()
    for k in range(nx):
        wide = jnp.dot(
            zr[k].reshape(eighth * seqs, zdim), placing, preferred_element_type=F32
        ).astype(BF16)
        for e in range(eighth):
            for p in range(pack):
                piece = wide[e * seqs : (e + 1) * seqs, p * zdim : (p + 1) * zdim]
                d = p * eighth + e
                for b in range(pack):
                    row = (k * pack + b) * seqs
                    rbd[row : row + seqs, d * zdim : (d + 1) * zdim] = jnp.where(
                        lane_block == b, piece, jnp.zeros_like(piece)
                    )
    for k in range(1, nx):
        gxc(lg, lg_s, lg_r, k).wait_recv()
    left = lg[...].reshape(nx * pack * seqs, grp * side)
    for e in range(eighth):
        cols = slice(e * pack * zdim, (e + 1) * pack * zdim)
        product = contract(left, rbd[:, cols], 0, 0).astype(BF16)
        for p in range(pack):
            d = e * pack + p
            for g in range(grp):
                osc[d * side : (d + 1) * side, g * zdim : (g + 1) * zdim] = product[
                    g * side : (g + 1) * side, p * zdim : (p + 1) * zdim
                ]
    for g in range(0, grp, 2):
        both = jnp.dot(
            wt[...], osc[:, g * zdim : (g + 2) * zdim], preferred_element_type=F32
        )
        middle = []
        for u in range(2):
            part = both[:, u * zdim : (u + 1) * zdim] * share[g + u : g + u + 1, :]
            pair_g = jnp.concatenate([pf[p * grp + g + u] for p in range(pack)], axis=0)
            middle.append(pair_g.astype(F32) + part.T)
        middle = jnp.concatenate(middle, axis=0)
        trans = standardize(middle).astype(BF16)
        expanded = jnp.maximum(
            jnp.dot(trans, ww[...], preferred_element_type=F32), 0.0
        ).astype(BF16)
        result = (middle + jnp.dot(expanded, wn[...], preferred_element_type=F32)).astype(BF16)
        for u in range(2):
            for p in range(pack):
                start = u * zdim + p * res
                pair_out[p * grp + g + u] = result[start : start + res]

    for c in range(chunks):
        for k in range(1, ny):
            hy(k, c).wait_send()
        for k in range(ny):
            for m in range(1, nz):
                hz(k, m, c).wait_send()
    for k in range(1, nr):
        ig(k).wait_send()
        mgc(k).wait_send()
    for k in range(1, nx):
        remote(mask, mx.at[q], mx_s.at[k - 1], mx_r.at[k - 1], {"gx": (q + k) % nx}).wait_send()
        gxc(bx, bx_s, bx_r, k).wait_send()
        gxc(lg, lg_s, lg_r, k).wait_send()
    for k in range(1, nr):
        spread_right(k).wait_send()

    @pl.when(q != r)
    def _():
        swap().wait_send()

    for k in range(nr):
        @pl.when(jnp.logical_or(q != r, r != k))
        def _():
            crossing(mask, mc, mc_s, mc_r, k).wait_send()


def solution(mesh):
    nx, ny, nz = mesh.shape["gx"], mesh.shape["gy"], mesh.shape["gz"]
    nr = ny * nz

    def local(*arrays):
        arrays = list(arrays)
        for index in (10, 11, 12):
            arrays[index] = arrays[index].T
        hp, pf, wb, w1, wm = arrays[1], arrays[3], arrays[10], arrays[11], arrays[13]
        seqs, res, depth = hp.shape
        zdim = pf.shape[2]
        heads, side = wb.shape[0], w1.shape[0]
        keys, pack = nr * res, zdim // res
        grp = res // pack
        chunk = pack
        chunks = seqs // chunk
        dma = pltpu.SemaphoreType.DMA
        vm = pltpu.VMEM
        scratch = [
            vm((nr, seqs, res, depth), BF16),
            vm((nr, seqs, res), jnp.int32),
            vm((nr, seqs, res), jnp.int32),
            vm((nx, seqs, res), jnp.int32),
            vm((nx, seqs, res), jnp.int32),
            vm((nx, heads, res * res), F32),
            vm((nx, pack * seqs, grp * side), BF16),
            vm((side // pack, seqs, zdim), BF16),
            vm((nx, side // pack, seqs, zdim), BF16),
            vm((seqs, keys), jnp.int32),
            vm((seqs, keys), F32),
            vm((heads, res, keys), F32),
            vm((seqs * res, depth), F32),
            vm((seqs * res, depth), BF16),
            vm((seqs * res, depth), F32),
            vm((seqs * res, zdim), F32),
            vm((side // pack, seqs, zdim), F32),
            vm((pack * seqs, grp * side), F32),
            vm((zdim, side * side), BF16),
            vm(wm.shape, F32),
            vm((nx * pack * seqs, side * zdim), BF16),
            vm((side * side, res * res), BF16),
            dma((max(ny - 1, 1), chunks)), dma((max(ny - 1, 1), chunks)),
            dma((ny, max(nz - 1, 1), chunks)), dma((ny, max(nz - 1, 1), chunks)),
            dma((nr,)), dma((nr,)), dma((nr,)), dma((nr,)),
            dma((nx,)), dma((nx,)), dma((nr,)), dma((nx,)),
            dma((nx,)), dma((nx,)), dma((nx,)), dma((nx,)),
            dma((nr,)), dma((nr,)), dma, dma, dma,
        ] + [vm(arrays[k].shape, BF16) for k in LATE] + [dma((len(LATE),))]
        return pl.pallas_call(
            functools.partial(kernel, (nx, ny, nz, chunk)),
            out_shape=(
                jax.ShapeDtypeStruct(hp.shape, BF16),
                jax.ShapeDtypeStruct(pf.shape, BF16),
            ),
            in_specs=[
                pl.BlockSpec(memory_space=pl.ANY if k in LATE else pltpu.VMEM)
                for k in range(len(arrays))
            ],
            out_specs=(pl.BlockSpec(memory_space=pltpu.VMEM),) * 2,
            scratch_shapes=scratch,
            compiler_params=pltpu.CompilerParams(
                collective_id=0, has_side_effects=True, vmem_limit_bytes=60 * 1024 * 1024
            ),
        )(*arrays)

    in_specs = (
        P(("grp", "gx"), ("gy", "gz")),
        P(("grp", "gx"), ("gy", "gz"), None),
        P(("grp", "gx"), ("gy", "gz")),
        P(("grp", "gy", "gz"), "gx", None),
    ) + (P(),) * 12
    out_specs = (P(("grp", "gx"), ("gy", "gz"), None), P(("grp", "gy", "gz"), "gx", None))
    return jax.shard_map(local, mesh=mesh, in_specs=in_specs, out_specs=out_specs, check_vma=False)
```
